64 devices in a mesh: rep: 4 (over x, y), shard: 16 (over z, core).
Axes of the slice: x: 2, y: 2, z: 8, core: 2. Of those that a mesh axis runs over, the one named last changes fastest.
The devices are a block of a 4x4x8 slice.
Arguments:
- ratings: float32 [4096, 8192], P(('rep', 'shard')), parts along dimension 0
- observed: int32 [4096, 8192], P(('rep', 'shard')), parts along dimension 0
- user_init: float32 [4096, 128], P(('rep', 'shard')), parts along dimension 0
- item_init: float32 [32768, 128], P(('rep', 'shard')), parts along dimension 0
Outputs:
- output 1: float32 [4096, 128], P(('rep', 'shard')), parts along dimension 0
- output 2: float32 [32768, 128], P(('rep', 'shard')), parts along dimension 0
There are 4 independent parts. The reference program is written for one: setup_inputs(seed, part) draws one part's arguments, and reference() takes and returns one part's arrays. A program takes and returns all parts, laid end to end along the dimension named above; each array names one.
All inputs are finite; a program needn't handle non-finite values.
Results may differ from the reference program's by a relative error of at most 0.00268177.
Values are sent between devices in bfloat16 or wider.
A program may use at most 768 MiB of HBM per device.

```python
import jax
import jax.numpy as jnp
import math
from jax import lax

GROUP_DEVS = 16
USERS_DEV = 64
ITEMS_DEV = 512
FACTOR_RANK = 128
STRATUM_STEPS = 4
EPOCHS = 2

USERS = USERS_DEV * GROUP_DEVS
ITEMS = ITEMS_DEV * GROUP_DEVS
STEP_SCALE = (USERS_DEV + ITEMS_DEV + FACTOR_RANK) / math.sqrt(FACTOR_RANK)
STEP_SIZE = 0.5 / STEP_SCALE
WEIGHT_DECAY = 0.03 * math.sqrt(USERS_DEV * ITEMS_DEV / FACTOR_RANK)


def setup_inputs(seed: int = 0, part: int = 0) -> dict:
    base_key = jax.random.fold_in(jax.random.key(seed), part)
    sub_keys = jax.random.split(base_key, 6)
    init_scale = FACTOR_RANK ** -0.25
    true_users = jax.random.normal(sub_keys[0], (USERS, FACTOR_RANK), jnp.float32) * init_scale
    true_items = jax.random.normal(sub_keys[1], (ITEMS, FACTOR_RANK), jnp.float32) * init_scale
    rating_noise = 0.3 * jax.random.normal(sub_keys[2], (USERS, ITEMS), jnp.float32)
    ratings = jnp.dot(true_users, true_items.T) + rating_noise
    observed = (jax.random.randint(sub_keys[3], (USERS, ITEMS), 0, 10) < 3).astype(jnp.int32)
    user_init = jax.random.normal(sub_keys[4], (USERS, FACTOR_RANK), jnp.float32) * init_scale
    item_init = jax.random.normal(sub_keys[5], (ITEMS, FACTOR_RANK), jnp.float32) * init_scale
    return {"ratings": ratings, "observed": observed, "user_init": user_init, "item_init": item_init}


def to_bf16(values):
    return values.astype(jnp.bfloat16).astype(jnp.float32)


def reference(ratings, observed, user_init, item_init):
    rating_grid = ratings.reshape(GROUP_DEVS, USERS_DEV, GROUP_DEVS, ITEMS_DEV)
    seen_grid = (observed != 0).reshape(GROUP_DEVS, USERS_DEV, GROUP_DEVS, ITEMS_DEV)
    dev_ids = jnp.arange(GROUP_DEVS)
    user_blocks = user_init.reshape(GROUP_DEVS, USERS_DEV, FACTOR_RANK)
    held_items = item_init.reshape(GROUP_DEVS, ITEMS_DEV, FACTOR_RANK)

    def stratum(loop_state, stratum_idx):
        user_now, held_now = loop_state
        col_ids = (dev_ids + stratum_idx) % GROUP_DEVS
        rating_blk = rating_grid[dev_ids, :, col_ids]
        seen_blk = seen_grid[dev_ids, :, col_ids]

        def step(state_pair, unused):
            user_cur, item_cur = state_pair
            item_bf = to_bf16(item_cur)
            predicted = jnp.einsum("pur,pir->pui", to_bf16(user_cur), item_bf)
            residual = to_bf16(jnp.where(seen_blk, predicted - rating_blk, 0.0))
            user_new = user_cur - STEP_SIZE * (jnp.einsum("pui,pir->pur", residual, item_bf) + WEIGHT_DECAY * user_cur)
            user_bf = to_bf16(user_new)
            predicted = jnp.einsum("pur,pir->pui", user_bf, item_bf)
            residual = to_bf16(jnp.where(seen_blk, predicted - rating_blk, 0.0))
            item_new = item_cur - STEP_SIZE * (jnp.einsum("pui,pur->pir", residual, user_bf) + WEIGHT_DECAY * item_cur)
            return (user_new, item_new), None

        (user_now, held_now), unused = lax.scan(step, (user_now, held_now), None, length=STRATUM_STEPS)
        held_now = jnp.roll(held_now, -1, axis=0)
        return (user_now, held_now), None

    stratum_order = jnp.tile(dev_ids, EPOCHS)
    (user_blocks, held_items), unused = lax.scan(stratum, (user_blocks, held_items), stratum_order)
    return user_blocks.reshape(USERS, FACTOR_RANK), held_items.reshape(ITEMS, FACTOR_RANK)
```

```python
import functools
import math

import jax
import jax.numpy as jnp
from jax import lax
from jax.experimental import pallas as pl
from jax.experimental.pallas import tpu as pltpu
from jax.sharding import PartitionSpec as P

STRATUM_STEPS = 4
EPOCHS = 2
QUAD = 4
AHEAD = 4
MESH = pl.DeviceIdType.MESH


def kernel(
    n, step_size, weight_decay, ratings, observed, user_in, item_in, user_out, item_out,
    rate_stage, seen_stage, code_send, code, items, users, items_bf,
    load_r, load_m, code_ss, code_rs, user_ss, user_rs, item_ss, item_rs,
):
    n_rows, rank = user_in.shape
    n_items = item_in.shape[0]
    strata = EPOCHS * n
    me = lax.axis_index("shard")
    lane = lax.rem(me, QUAD)
    base = me - lane
    ahead_dev = lax.rem(me + QUAD, n)
    back_dev = lax.rem(me + n - QUAD, n)

    def mate(offset):
        return base + lax.rem(lane + offset, QUAD)

    def loads(t):
        col = pl.multiple_of(lax.rem(me + t, n) * n_items, n_items)
        return (
            pltpu.make_async_copy(ratings.at[:, pl.ds(col, n_items)], rate_stage.at[t], load_r.at[t]),
            pltpu.make_async_copy(observed.at[:, pl.ds(col, n_items)], seen_stage.at[t], load_m.at[t]),
        )

    def code_copy(t, offset):
        return pltpu.make_async_remote_copy(
            src_ref=code_send.at[t], dst_ref=code.at[t], send_sem=code_ss.at[t], recv_sem=code_rs.at[t],
            device_id={"shard": mate(offset)}, device_id_type=MESH)

    def user_copy(t):
        return pltpu.make_async_remote_copy(
            src_ref=users.at[t], dst_ref=users.at[t + 1], send_sem=user_ss.at[t], recv_sem=user_rs.at[t],
            device_id={"shard": mate(1)}, device_id_type=MESH)

    def item_copy(k):
        return pltpu.make_async_remote_copy(
            src_ref=items.at[k], dst_ref=items.at[k + 1], send_sem=item_ss.at[k], recv_sem=item_rs.at[k],
            device_id={"shard": back_dev}, device_id_type=MESH)

    def coded(t):
        return jnp.where(seen_stage[t] != 0, rate_stage[t], jnp.inf)

    def make_code(t, offset):
        for load in loads(t):
            load.wait()
        if offset == 0:
            code[t] = coded(t)
        else:
            code_send[t] = coded(t)
            code_copy(t, offset).start()

    @pl.loop(0, n)
    def _(t):
        for load in loads(t):
            load.start()

    barrier = pltpu.get_barrier_semaphore()
    greeted = [mate(1), mate(2), mate(3), ahead_dev, back_dev]
    for dev in greeted:
        pl.semaphore_signal(barrier, inc=1, device_id={"shard": dev}, device_id_type=MESH)

    users[0] = user_in[...]
    items[0] = item_in[...].T
    items_bf[...] = items[0].astype(jnp.bfloat16)
    pl.semaphore_wait(barrier, len(greeted))
    for t in range(AHEAD):
        make_code(t, t % QUAD)

    def stratum(t, offset, coding):
        turns = (t - lane + QUAD - 1) // QUAD
        first = lax.rem(lane + QUAD - offset, QUAD) == QUAD - 1
        last = lax.rem(lane + QUAD - offset, QUAD) == 0

        @pl.when(jnp.logical_and(first, t > 0))
        def _():
            item_copy(turns - 1).wait_recv()
            items_bf[...] = items[turns].astype(jnp.bfloat16)

        if coding:
            make_code(t + AHEAD, (offset + AHEAD) % QUAD)
            if offset != 0:
                code_copy(t, offset).wait_recv()

        @pl.when(t > 0)
        def _():
            user_copy(t - 1).wait_recv()

        user = users[t]
        user_bf = user.astype(jnp.bfloat16)
        for step in range(STRATUM_STEPS):
            pred = jnp.dot(user_bf, items_bf[...], preferred_element_type=jnp.float32)
            rate = code[lax.rem(t, n)]
            err = jnp.where(rate < jnp.inf, pred - rate, 0.0).astype(jnp.bfloat16)
            grad = lax.dot_general(err, items_bf[...], (((1,), (1,)), ((), ())), preferred_element_type=jnp.float32)
            user = user - step_size * (grad + weight_decay * user)
            user_bf = user.astype(jnp.bfloat16)
            if step == STRATUM_STEPS - 1:
                users[t] = user
                user_copy(t).start()
            pred = jnp.dot(user_bf, items_bf[...], preferred_element_type=jnp.float32)
            rate = code[lax.rem(t, n)]
            err = jnp.where(rate < jnp.inf, pred - rate, 0.0).astype(jnp.bfloat16)
            grad = lax.dot_general(user_bf, err, (((0,), (0,)), ((), ())), preferred_element_type=jnp.float32)
            item = items[turns]
            item = item - step_size * (grad + weight_decay * item)
            items[turns] = item
            items_bf[...] = item.astype(jnp.bfloat16)

        @pl.when(last)
        def _():
            item_copy(turns).start()

    @pl.loop(0, (n - AHEAD) // QUAD)
    def _(rnd):
        for offset in range(QUAD):
            stratum(rnd * QUAD + offset, offset, True)

    @pl.loop((n - AHEAD) // QUAD, strata // QUAD)
    def _(rnd):
        for offset in range(QUAD):
            t = rnd * QUAD + offset
            if offset != 0:
                @pl.when(t < n)
                def _():
                    code_copy(t, offset).wait_recv()
            stratum(t, offset, False)

    shifts = strata // QUAD

    @pl.when(lane == QUAD - 1)
    def _():
        item_copy(shifts - 1).wait_recv()

    item_out[...] = items[shifts]
    user_copy(strata - 1).wait_recv()
    user_out[...] = users[strata]

    @pl.loop(0, strata)
    def _(t):
        user_copy(t).wait_send()

    @pl.loop(0, shifts)
    def _(k):
        item_copy(k).wait_send()

    @pl.loop(0, n // QUAD)
    def _(rnd):
        for offset in range(1, QUAD):
            code_copy(rnd * QUAD + offset, offset).wait_send()


def solution(mesh):
    n = mesh.shape["shard"]
    row_spec = P(("rep", "shard"), None)

    def local(ratings, observed, user_init, item_init):
        users_dev = ratings.shape[0]
        items_dev, rank = item_init.shape
        step_size = 0.5 / ((users_dev + items_dev + rank) / math.sqrt(rank))
        weight_decay = 0.03 * math.sqrt(users_dev * items_dev / rank)
        strata = EPOCHS * n
        shifts = strata // QUAD
        vmem = pl.BlockSpec(memory_space=pltpu.VMEM)
        anywhere = pl.BlockSpec(memory_space=pl.ANY)
        dma = pltpu.SemaphoreType.DMA
        user_out, item_out = pl.pallas_call(
            functools.partial(kernel, n, step_size, weight_decay),
            out_shape=(
                jax.ShapeDtypeStruct((users_dev, rank), jnp.float32),
                jax.ShapeDtypeStruct((rank, items_dev), jnp.float32),
            ),
            in_specs=[anywhere, anywhere, vmem, vmem],
            out_specs=(vmem, vmem),
            scratch_shapes=[
                pltpu.VMEM((n, users_dev, items_dev), jnp.float32),
                pltpu.VMEM((n, users_dev, items_dev), jnp.int32),
                pltpu.VMEM((n, users_dev, items_dev), jnp.float32),
                pltpu.VMEM((n, users_dev, items_dev), jnp.float32),
                pltpu.VMEM((shifts + 1, rank, items_dev), jnp.float32),
                pltpu.VMEM((strata + 1, users_dev, rank), jnp.float32),
                pltpu.VMEM((rank, items_dev), jnp.bfloat16),
                dma((n,)), dma((n,)), dma((n,)), dma((n,)),
                dma((strata,)), dma((strata,)), dma((shifts,)), dma((shifts,)),
            ],
            compiler_params=pltpu.CompilerParams(collective_id=0, has_side_effects=True),
        )(ratings, observed, user_init, item_init)
        return user_out, item_out.T

    return jax.shard_map(local, mesh=mesh, in_specs=(row_spec,) * 4, out_specs=(row_spec, row_spec), check_vma=False)
```

```python
import functools
import math

import jax
import jax.numpy as jnp
from jax import lax
from jax.experimental import pallas as pl
from jax.experimental.pallas import tpu as pltpu
from jax.sharding import PartitionSpec as P

STRATUM_STEPS = 4
EPOCHS = 2
AHEAD = 2
AHEAD_DOWN = 4
MESH = pl.DeviceIdType.MESH


def kernel(
    n, step_size, weight_decay, ratings, observed, user_in, item_in, user_out, item_out,
    rate_stage, seen_stage, code_send, code, items, items_bf, users,
    load_r, load_m, code_ss, code_rs, user_ss, user_rs,
):
    n_items = item_in.shape[0]
    strata = EPOCHS * n
    half = n // 2
    me = lax.axis_index("shard")

    def up(offset):
        return {"shard": lax.rem(me + offset, n)}

    def loads(t):
        col = pl.multiple_of(lax.rem(me + t, n) * n_items, n_items)
        return (
            pltpu.make_async_copy(ratings.at[:, pl.ds(col, n_items)], rate_stage.at[t], load_r.at[t]),
            pltpu.make_async_copy(observed.at[:, pl.ds(col, n_items)], seen_stage.at[t], load_m.at[t]),
        )

    def code_copy(t):
        return pltpu.make_async_remote_copy(
            src_ref=code_send.at[t], dst_ref=code.at[t], send_sem=code_ss.at[t], recv_sem=code_rs.at[t],
            device_id=up(t), device_id_type=MESH)

    def user_copy(t):
        return pltpu.make_async_remote_copy(
            src_ref=users.at[t], dst_ref=users.at[t + 1], send_sem=user_ss.at[t], recv_sem=user_rs.at[t],
            device_id=up(1), device_id_type=MESH)

    def coded(t):
        for load in loads(t):
            load.wait()
        return jnp.where(seen_stage[t] != 0, rate_stage[t], jnp.inf)

    def send_code(t):
        code_send[t] = coded(t)
        code_copy(t).start()

    @pl.loop(0, n)
    def _(t):
        for load in loads(t):
            load.start()

    barrier = pltpu.get_barrier_semaphore()
    for offset in range(1, n):
        pl.semaphore_signal(barrier, inc=1, device_id=up(offset), device_id_type=MESH)

    users[0] = user_in[...]
    items[...] = item_in[...].T
    items_bf[...] = items[...].astype(jnp.bfloat16)
    code[0] = coded(0)
    pl.semaphore_wait(barrier, n - 1)
    for t in range(1, AHEAD):
        send_code(t)

    @pl.loop(0, strata)
    def _(t):
        @pl.when(t + AHEAD <= half)
        def _():
            send_code(t + AHEAD)

        @pl.when(jnp.logical_and(t + AHEAD_DOWN > half, t + AHEAD_DOWN < n))
        def _():
            send_code(t + AHEAD_DOWN)

        @pl.when(jnp.logical_and(t > 0, t < n))
        def _():
            code_copy(t).wait_recv()

        @pl.when(t > 0)
        def _():
            user_copy(t - 1).wait_recv()

        slot = lax.rem(t, n)
        user = users[t]
        user_bf = user.astype(jnp.bfloat16)
        for step in range(STRATUM_STEPS):
            pred = jnp.dot(user_bf, items_bf[...], preferred_element_type=jnp.float32)
            rate = code[slot]
            err = jnp.where(rate < jnp.inf, pred - rate, 0.0).astype(jnp.bfloat16)
            grad = lax.dot_general(err, items_bf[...], (((1,), (1,)), ((), ())), preferred_element_type=jnp.float32)
            user = user - step_size * (grad + weight_decay * user)
            user_bf = user.astype(jnp.bfloat16)
            if step == STRATUM_STEPS - 1:
                users[t] = user
                user_copy(t).start()
            pred = jnp.dot(user_bf, items_bf[...], preferred_element_type=jnp.float32)
            rate = code[slot]
            err = jnp.where(rate < jnp.inf, pred - rate, 0.0).astype(jnp.bfloat16)
            grad = lax.dot_general(user_bf, err, (((0,), (0,)), ((), ())), preferred_element_type=jnp.float32)
            item = items[...]
            item = item - step_size * (grad + weight_decay * item)
            items[...] = item
            items_bf[...] = item.astype(jnp.bfloat16)

    item_out[...] = items[...]
    user_copy(strata - 1).wait_recv()
    user_out[...] = users[strata]

    @pl.loop(0, strata)
    def _(t):
        user_copy(t).wait_send()

    @pl.loop(1, n)
    def _(t):
        code_copy(t).wait_send()


def solution(mesh):
    n = mesh.shape["shard"]
    row_spec = P(("rep", "shard"), None)

    def local(ratings, observed, user_init, item_init):
        users_dev = ratings.shape[0]
        items_dev, rank = item_init.shape
        step_size = 0.5 / ((users_dev + items_dev + rank) / math.sqrt(rank))
        weight_decay = 0.03 * math.sqrt(users_dev * items_dev / rank)
        strata = EPOCHS * n
        vmem = pl.BlockSpec(memory_space=pltpu.VMEM)
        anywhere = pl.BlockSpec(memory_space=pl.ANY)
        dma = pltpu.SemaphoreType.DMA
        user_out, item_out = pl.pallas_call(
            functools.partial(kernel, n, step_size, weight_decay),
            out_shape=(
                jax.ShapeDtypeStruct((users_dev, rank), jnp.float32),
                jax.ShapeDtypeStruct((rank, items_dev), jnp.float32),
            ),
            in_specs=[anywhere, anywhere, vmem, vmem],
            out_specs=(vmem, vmem),
            scratch_shapes=[
                pltpu.VMEM((n, users_dev, items_dev), jnp.float32),
                pltpu.VMEM((n, users_dev, items_dev), jnp.int32),
                pltpu.VMEM((n, users_dev, items_dev), jnp.float32),
                pltpu.VMEM((n, users_dev, items_dev), jnp.float32),
                pltpu.VMEM((rank, items_dev), jnp.float32),
                pltpu.VMEM((rank, items_dev), jnp.bfloat16),
                pltpu.VMEM((strata + 1, users_dev, rank), jnp.float32),
                dma((n,)), dma((n,)), dma((n,)), dma((n,)), dma((strata,)), dma((strata,)),
            ],
            compiler_params=pltpu.CompilerParams(collective_id=0, has_side_effects=True),
        )(ratings, observed, user_init, item_init)
        return user_out, item_out.T

    return jax.shard_map(local, mesh=mesh, in_specs=(row_spec,) * 4, out_specs=(row_spec, row_spec), check_vma=False)
```

```python
import functools
import math

import jax
import jax.numpy as jnp
from jax import lax
from jax.experimental import pallas as pl
from jax.experimental.pallas import tpu as pltpu
from jax.sharding import PartitionSpec as P

STRATUM_STEPS = 4
EPOCHS = 2
CORES = 2
RELAY_HOP = 4
SEND_AT = {1: 0, 2: 0, 3: 1, 4: 3, 5: 2, 6: 4, 7: 0, 8: 0, 9: 4, 10: 1, 11: 7, 12: 8, 13: 9, 14: 13, 15: 12, 16: 14}
RELAY_AT = {7: 1, 8: 2}
MESH = pl.DeviceIdType.MESH


def kernel(
    n, step_size, weight_decay, ratings, observed, user_in, item_in, user_out, item_out,
    rate_stage, seen_stage, code_send, code, relay, item_stage, items, items_bf, users,
    load_r, load_m, load_i, load_u, code_ss, code_rs, relay_ss, relay_rs, user_ss, user_rs,
    item_ss, item_rs, bf_ss, bf_rs,
):
    n_items = item_in.shape[0]
    strata = EPOCHS * n
    chips = n // CORES
    me = lax.axis_index("shard")
    chip = me // CORES
    core = lax.rem(me, CORES)
    odd_chip = lax.rem(chip, 2)
    partner = me + 1 - 2 * core
    relayed = sorted(RELAY_AT)

    def at(device):
        return {"shard": device}

    def block_place(owner, b):
        item = lax.rem(owner + b, n)
        return item - lax.rem(item, 2) + lax.rem(owner + item // 2, 2)

    def loads(b):
        col = pl.multiple_of(lax.rem(me + b, n) * n_items, n_items)
        slot = b % n
        return (
            pltpu.make_async_copy(ratings.at[:, pl.ds(col, n_items)], rate_stage.at[slot], load_r.at[slot]),
            pltpu.make_async_copy(observed.at[:, pl.ds(col, n_items)], seen_stage.at[slot], load_m.at[slot]),
        )

    def code_copy(b):
        return pltpu.make_async_remote_copy(
            src_ref=code_send.at[b], dst_ref=code.at[b], send_sem=code_ss.at[b], recv_sem=code_rs.at[b],
            device_id=at(block_place(me, b)), device_id_type=MESH)

    def relay_in(b):
        r = relayed.index(b)
        return pltpu.make_async_remote_copy(
            src_ref=code_send.at[b], dst_ref=relay.at[r], send_sem=relay_ss.at[r], recv_sem=relay_rs.at[r],
            device_id=at(lax.rem(me + n - RELAY_HOP, n)), device_id_type=MESH)

    def relay_out(b):
        return pltpu.make_async_remote_copy(
            src_ref=relay.at[relayed.index(b)], dst_ref=code.at[b], send_sem=code_ss.at[b], recv_sem=code_rs.at[b],
            device_id=at(block_place(lax.rem(me + RELAY_HOP, n), b)), device_id_type=MESH)

    def user_copy(t, device):
        return pltpu.make_async_remote_copy(
            src_ref=users.at[t], dst_ref=users.at[t + 1], send_sem=user_ss.at[t], recv_sem=user_rs.at[t],
            device_id=at(device), device_id_type=MESH)

    def bf_copy(t):
        return pltpu.make_async_remote_copy(
            src_ref=items_bf.at[t], dst_ref=items_bf.at[t + 1], send_sem=bf_ss.at[t], recv_sem=bf_rs.at[t],
            device_id=at(partner), device_id_type=MESH)

    def item_copy(t):
        return pltpu.make_async_remote_copy(
            src_ref=items.at[t], dst_ref=items.at[t + 1], send_sem=item_ss.at[t], recv_sem=item_rs.at[t],
            device_id=at(partner), device_id_type=MESH)

    def item_half(t):
        if isinstance(t, int) and t in (0, strata):
            return core
        return lax.rem(core + t + chip, 2)

    def user_next(t):
        half = item_half(t)
        up = lax.rem(chip + half, chips)
        shift = t + 1
        if isinstance(t, int) and t + 1 == strata:
            return CORES * up + lax.rem(1 - half + shift, 2)
        return CORES * up + lax.rem(1 - half + shift + up, 2)

    def owner_of(t):
        return lax.rem(CORES * chip + item_half(t) + strata - t, n)

    first_item = pltpu.make_async_copy(item_in, item_stage, load_i)
    first_user = pltpu.make_async_copy(user_in, users.at[0], load_u)

    def coded(b):
        return jnp.where(seen_stage[b % n] != 0, rate_stage[b % n], jnp.inf)

    def send_code(b):
        if b < n:
            for load in loads(b):
                load.wait()
        if b in (1, n - 1, n):
            stays = block_place(me, b) == me

            @pl.when(stays)
            def _():
                code[b] = coded(b)

            @pl.when(jnp.logical_not(stays))
            def _():
                code_send[b] = coded(b)
                code_copy(b).start()
        else:
            code_send[b] = coded(b)
            (relay_in if b in relayed else code_copy)(b).start()

    def traffic(t):
        for when in sorted(set(SEND_AT.values())):
            @pl.when(t == when)
            def _():
                for b in sorted(SEND_AT):
                    if SEND_AT[b] == when:
                        send_code(b)
        for b in relayed:
            @pl.when(t == RELAY_AT[b])
            def _():
                relay_in(b).wait_recv()
                relay_out(b).start()

    barrier = pltpu.get_barrier_semaphore()
    for offset in range(1, n):
        pl.semaphore_signal(barrier, inc=1, device_id=at(lax.rem(me + offset, n)), device_id_type=MESH)
    first_item.start()
    for load in loads(0):
        load.start()
    first_user.start()
    for b in sorted(range(1, n), key=lambda b: SEND_AT[b]):
        for load in loads(b):
            load.start()
    first_item.wait()
    first = item_stage[...].T
    items[0] = first
    items_bf[0] = first.astype(jnp.bfloat16)
    for load in loads(0):
        load.wait()
    code[0] = coded(0)
    pl.semaphore_wait(barrier, n - 1)

    def stratum(t):
        fixed = isinstance(t, int)
        start, end = fixed and t == 0, fixed and t == strata - 1
        half = item_half(t)
        target = user_next(t)
        user_stays = target == me
        item_stays = odd_chip if start or end else 0
        user_from_far = half == 0
        if fixed and t == 1:
            user_from_far = jnp.logical_or(user_from_far, odd_chip == 1)
        item_swapped = odd_chip == 0 if fixed and t == 1 else None

        if not (fixed and t > n):
            pl.when(t <= n)(functools.partial(traffic, t))

            @pl.when(jnp.logical_and(jnp.logical_and(t > 0, t <= n), owner_of(t) != me))
            def _():
                code_copy(t).wait_recv()

        if start:
            first_user.wait()
        else:
            @pl.when(user_from_far)
            def _():
                user_copy(t - 1, partner).wait_recv()

            if item_swapped is None:
                bf_copy(t - 1).wait_recv()
            else:
                @pl.when(item_swapped)
                def _():
                    bf_copy(t - 1).wait_recv()
                    item_copy(t - 1).wait_recv()

        slot = jnp.where(t > n, t - n, t)
        user = users[t]
        user_bf = user.astype(jnp.bfloat16)
        for step in range(STRATUM_STEPS):
            final = step == STRATUM_STEPS - 1
            pred = jnp.dot(user_bf, items_bf[t], preferred_element_type=jnp.float32)
            rate = code[slot]
            err = jnp.where(rate < jnp.inf, pred - rate, 0.0).astype(jnp.bfloat16)
            user = (1.0 - step_size * weight_decay) * user
            for h in range(2):
                cols = slice(h * n_items // 2, (h + 1) * n_items // 2)
                grad = lax.dot_general(
                    err[:, cols], items_bf[t, :, cols], (((1,), (1,)), ((), ())), preferred_element_type=jnp.float32)
                user = user - step_size * grad
            user_bf = user.astype(jnp.bfloat16)
            if final:
                users[t + user_stays.astype(jnp.int32)] = user

                @pl.when(jnp.logical_not(user_stays))
                def _():
                    user_copy(t, target).start()
            pred = jnp.dot(user_bf, items_bf[t], preferred_element_type=jnp.float32)
            rate = code[slot]
            err = jnp.where(rate < jnp.inf, pred - rate, 0.0).astype(jnp.bfloat16)
            grad = lax.dot_general(user_bf, err, (((0,), (0,)), ((), ())), preferred_element_type=jnp.float32)
            if step == 0 and not start and item_swapped is None:
                item_copy(t - 1).wait_recv()
            item = (1.0 - step_size * weight_decay) * items[t] - step_size * grad
            out = t + item_stays if final else t
            if not (final and end):
                items_bf[out] = item.astype(jnp.bfloat16)
            items[out] = item

        if start or end:
            @pl.when(item_stays == 0)
            def _():
                if start:
                    bf_copy(t).start()
                item_copy(t).start()
        else:
            bf_copy(t).start()
            item_copy(t).start()

    stratum(0)
    stratum(1)
    pl.loop(2, strata - 1)(stratum)
    stratum(strata - 1)

    @pl.when(odd_chip == 0)
    def _():
        item_copy(strata - 1).wait_recv()

    item_out[...] = items[strata]

    @pl.when(jnp.logical_or(core == 0, odd_chip == 1))
    def _():
        user_copy(strata - 1, partner).wait_recv()

    user_out[...] = users[strata]

    def drain(t):
        @pl.when(user_next(t) != me)
        def _():
            user_copy(t, partner).wait_send()

        if isinstance(t, int):
            @pl.when(odd_chip == 0)
            def _():
                if t == 0:
                    bf_copy(t).wait_send()
                item_copy(t).wait_send()
        else:
            bf_copy(t).wait_send()
            item_copy(t).wait_send()

    drain(0)
    pl.loop(1, strata - 1)(drain)
    drain(strata - 1)

    @pl.loop(1, n + 1)
    def _(b):
        @pl.when(block_place(me, b) != me)
        def _():
            code_copy(b).wait_send()

    for b in relayed:
        relay_in(b).wait_send()


def solution(mesh):
    n = mesh.shape["shard"]
    row_spec = P(("rep", "shard"), None)

    def local(ratings, observed, user_init, item_init):
        users_dev = ratings.shape[0]
        items_dev, rank = item_init.shape
        step_size = 0.5 / ((users_dev + items_dev + rank) / math.sqrt(rank))
        weight_decay = 0.03 * math.sqrt(users_dev * items_dev / rank)
        strata = EPOCHS * n
        relays = max(1, len(RELAY_AT))
        vmem = pl.BlockSpec(memory_space=pltpu.VMEM)
        anywhere = pl.BlockSpec(memory_space=pl.ANY)
        dma = pltpu.SemaphoreType.DMA
        user_out, item_out = pl.pallas_call(
            functools.partial(kernel, n, step_size, weight_decay),
            out_shape=(
                jax.ShapeDtypeStruct((users_dev, rank), jnp.float32),
                jax.ShapeDtypeStruct((rank, items_dev), jnp.float32),
            ),
            in_specs=[anywhere] * 4,
            out_specs=(vmem, vmem),
            scratch_shapes=[
                pltpu.VMEM((n, users_dev, items_dev), jnp.float32),
                pltpu.VMEM((n, users_dev, items_dev), jnp.int32),
                pltpu.VMEM((n + 1, users_dev, items_dev), jnp.float32),
                pltpu.VMEM((n + 1, users_dev, items_dev), jnp.float32),
                pltpu.VMEM((relays, users_dev, items_dev), jnp.float32),
                pltpu.VMEM((items_dev, rank), jnp.float32),
                pltpu.VMEM((strata + 1, rank, items_dev), jnp.float32),
                pltpu.VMEM((strata, rank, items_dev), jnp.bfloat16),
                pltpu.VMEM((strata + 1, users_dev, rank), jnp.float32),
                dma((n,)), dma((n,)), dma, dma, dma((n + 1,)), dma((n + 1,)), dma((relays,)), dma((relays,)),
                dma((strata,)), dma((strata,)), dma((strata,)), dma((strata,)), dma((strata,)), dma((strata,)),
            ],
            compiler_params=pltpu.CompilerParams(collective_id=0, has_side_effects=True),
        )(ratings, observed, user_init, item_init)
        return user_out, item_out.T

    return jax.shard_map(local, mesh=mesh, in_specs=(row_spec,) * 4, out_specs=(row_spec, row_spec), check_vma=False)
```

```python
import functools
import math

import jax
import jax.numpy as jnp
from jax import lax
from jax.experimental import pallas as pl
from jax.experimental.pallas import tpu as pltpu
from jax.sharding import PartitionSpec as P

STRATUM_STEPS = 4
EPOCHS = 2
CORES = 2
PIECES = 1
SEND_AT = {(1, 0): 0, (2, 0): 1, (3, 0): 0, (4, 0): 2, (5, 0): 3, (6, 0): 5, (7, 0): 1, (8, 0): 3, (9, 0): 6, (10, 0): 0, (11, 0): 7, (12, 0): 7, (13, 0): 10, (14, 0): 13, (15, 0): 11, (16, 0): 14}
RELAY = {(7, 0): (4, 4), (8, 0): (4, 5)}
MESH = pl.DeviceIdType.MESH


def kernel(
    n, step_size, weight_decay, ratings, observed, user_in, item_in, user_out, item_out,
    rate_stage, seen_stage, code_send, code, relay, item_stage, items, items_bf, users,
    load_r, load_m, load_i, load_u, code_ss, code_rs, relay_ss, relay_rs, user_ss, user_rs,
    item_ss, item_rs, bf_ss, bf_rs,
):
    n_items = item_in.shape[0]
    rows = user_in.shape[0] // PIECES
    strata = EPOCHS * n
    chips = n // CORES
    me = lax.axis_index("shard")
    chip = me // CORES
    core = lax.rem(me, CORES)
    odd_chip = lax.rem(chip, 2)
    partner = me + 1 - 2 * core
    relayed = sorted(RELAY)

    def at(device):
        return {"shard": device}

    def shifted(offset):
        return at(lax.rem(me + n + offset, n))

    def block_place(owner, b):
        item = lax.rem(owner + b, n)
        return item - lax.rem(item, 2) + lax.rem(owner + item // 2, 2)

    def loads(b):
        col = pl.multiple_of(lax.rem(me + b, n) * n_items, n_items)
        slot = b % n
        return (
            pltpu.make_async_copy(ratings.at[:, pl.ds(col, n_items)], rate_stage.at[slot], load_r.at[slot]),
            pltpu.make_async_copy(observed.at[:, pl.ds(col, n_items)], seen_stage.at[slot], load_m.at[slot]),
        )

    def part(h):
        return pl.ds(h * rows, rows)

    def code_copy(b, h, device):
        return pltpu.make_async_remote_copy(
            src_ref=code_send.at[b, part(h)], dst_ref=code.at[b, part(h)], send_sem=code_ss.at[b, h],
            recv_sem=code_rs.at[b, h], device_id=at(device), device_id_type=MESH)

    def relay_in(b, h):
        r = relayed.index((b, h))
        return pltpu.make_async_remote_copy(
            src_ref=code_send.at[b, part(h)], dst_ref=relay.at[r], send_sem=relay_ss.at[r], recv_sem=relay_rs.at[r],
            device_id=shifted(-RELAY[b, h][0]), device_id_type=MESH)

    def relay_out(b, h):
        owner = lax.rem(me + RELAY[b, h][0], n)
        return pltpu.make_async_remote_copy(
            src_ref=relay.at[relayed.index((b, h))], dst_ref=code.at[b, part(h)], send_sem=code_ss.at[b, h],
            recv_sem=code_rs.at[b, h], device_id=at(block_place(owner, b)), device_id_type=MESH)

    def user_copy(t, device):
        return pltpu.make_async_remote_copy(
            src_ref=users.at[t], dst_ref=users.at[t + 1], send_sem=user_ss.at[t], recv_sem=user_rs.at[t],
            device_id=at(device), device_id_type=MESH)

    def bf_copy(t):
        return pltpu.make_async_remote_copy(
            src_ref=items_bf.at[t], dst_ref=items_bf.at[t + 1], send_sem=bf_ss.at[t], recv_sem=bf_rs.at[t],
            device_id=at(partner), device_id_type=MESH)

    def item_copy(t):
        return pltpu.make_async_remote_copy(
            src_ref=items.at[t], dst_ref=items.at[t + 1], send_sem=item_ss.at[t], recv_sem=item_rs.at[t],
            device_id=at(partner), device_id_type=MESH)

    def item_half(t):
        if isinstance(t, int) and t in (0, strata):
            return core
        return lax.rem(core + t + chip, 2)

    def user_next(t):
        half = item_half(t)
        up = lax.rem(chip + half, chips)
        if isinstance(t, int) and t + 1 == strata:
            return CORES * up + lax.rem(1 - half + t + 1, 2)
        return CORES * up + lax.rem(1 - half + t + 1 + up, 2)

    def owner_of(t):
        return lax.rem(CORES * chip + item_half(t) + strata - t, n)

    first_item = pltpu.make_async_copy(item_in, item_stage, load_i)
    first_user = pltpu.make_async_copy(user_in, users.at[0], load_u)

    def coded(b, h):
        return jnp.where(seen_stage[b % n, part(h)] != 0, rate_stage[b % n, part(h)], jnp.inf)

    def send_code(b, h):
        if b < n and all(SEND_AT[b, h] < SEND_AT[b, g] or (SEND_AT[b, h] == SEND_AT[b, g] and h <= g) for g in range(PIECES)):
            for load in loads(b):
                load.wait()
        if b in (1, n - 1, n):
            stays = block_place(me, b) == me

            @pl.when(stays)
            def _():
                code[b, part(h)] = coded(b, h)

            @pl.when(jnp.logical_not(stays))
            def _():
                code_send[b, part(h)] = coded(b, h)
                code_copy(b, h, block_place(me, b)).start()
        else:
            code_send[b, part(h)] = coded(b, h)
            if (b, h) in relayed:
                relay_in(b, h).start()
            else:
                code_copy(b, h, block_place(me, b)).start()

    def send_all(when):
        for b, h in sorted(SEND_AT):
            if SEND_AT[b, h] == when:
                send_code(b, h)

    def traffic(t):
        for when in sorted(set(SEND_AT.values()) - {0}):
            pl.when(t == when)(functools.partial(send_all, when))
        for b, h in relayed:
            @pl.when(t == RELAY[b, h][1])
            def _():
                relay_in(b, h).wait_recv()
                relay_out(b, h).start()

    barrier = pltpu.get_barrier_semaphore()
    for offset in range(1, n):
        pl.semaphore_signal(barrier, inc=1, device_id=shifted(offset), device_id_type=MESH)
    order = sorted(range(1, n), key=lambda b: min(SEND_AT[b, h] for h in range(PIECES)))
    early = [b for b in order if min(SEND_AT[b, h] for h in range(PIECES)) == 0]
    for b in early + [0]:
        for load in loads(b):
            load.start()
    first_item.start()
    first_user.start()
    for b in order[len(early):]:
        for load in loads(b):
            load.start()
    first_item.wait()
    first = item_stage[...].T
    items[0] = first
    items_bf[0] = first.astype(jnp.bfloat16)
    for load in loads(0):
        load.wait()
    for h in range(PIECES):
        code[0, part(h)] = coded(0, h)
    pl.semaphore_wait(barrier, n - 1)
    send_all(0)

    def stratum(t):
        fixed = isinstance(t, int)
        start, end = fixed and t == 0, fixed and t == strata - 1
        half = item_half(t)
        target = user_next(t)
        user_stays = target == me
        item_stays = odd_chip if start or end else 0
        user_from_far = half == 0
        if fixed and t == 1:
            user_from_far = jnp.logical_or(user_from_far, odd_chip == 1)
        item_swapped = odd_chip == 0 if fixed and t == 1 else None

        if not start and not (fixed and t > n):
            pl.when(t <= n)(functools.partial(traffic, t))

            @pl.when(jnp.logical_and(t <= n, owner_of(t) != me))
            def _():
                for h in range(PIECES):
                    code_copy(t, h, partner).wait_recv()

        if start:
            first_user.wait()
        else:
            @pl.when(user_from_far)
            def _():
                user_copy(t - 1, partner).wait_recv()

            if item_swapped is None:
                bf_copy(t - 1).wait_recv()
            else:
                @pl.when(item_swapped)
                def _():
                    bf_copy(t - 1).wait_recv()
                    item_copy(t - 1).wait_recv()

        slot = jnp.where(t > n, t - n, t)
        user = users[t]
        user_bf = user.astype(jnp.bfloat16)
        for step in range(STRATUM_STEPS):
            final = step == STRATUM_STEPS - 1
            pred = jnp.dot(user_bf, items_bf[t], preferred_element_type=jnp.float32)
            rate = code[slot]
            err = jnp.where(rate < jnp.inf, pred - rate, 0.0).astype(jnp.bfloat16)
            user = (1.0 - step_size * weight_decay) * user
            for h in range(2):
                cols = slice(h * n_items // 2, (h + 1) * n_items // 2)
                grad = lax.dot_general(
                    err[:, cols], items_bf[t, :, cols], (((1,), (1,)), ((), ())), preferred_element_type=jnp.float32)
                user = user - step_size * grad
            user_bf = user.astype(jnp.bfloat16)
            if final:
                users[t + user_stays.astype(jnp.int32)] = user

                @pl.when(jnp.logical_not(user_stays))
                def _():
                    user_copy(t, target).start()
            pred = jnp.dot(user_bf, items_bf[t], preferred_element_type=jnp.float32)
            rate = code[slot]
            err = jnp.where(rate < jnp.inf, pred - rate, 0.0).astype(jnp.bfloat16)
            grad = lax.dot_general(user_bf, err, (((0,), (0,)), ((), ())), preferred_element_type=jnp.float32)
            if step == 0 and not start and item_swapped is None:
                item_copy(t - 1).wait_recv()
            item = (1.0 - step_size * weight_decay) * items[t] - step_size * grad
            out = t + item_stays if final else t
            if not (final and end):
                items_bf[out] = item.astype(jnp.bfloat16)
            items[out] = item

        if start or end:
            @pl.when(item_stays == 0)
            def _():
                if start:
                    bf_copy(t).start()
                item_copy(t).start()
        else:
            bf_copy(t).start()
            item_copy(t).start()

    stratum(0)
    stratum(1)
    pl.loop(2, strata - 1)(stratum)
    stratum(strata - 1)

    def drain(t):
        @pl.when(user_next(t) != me)
        def _():
            user_copy(t, partner).wait_send()

        bf_copy(t).wait_send()
        item_copy(t).wait_send()

    pl.loop(1, strata - 1)(drain)

    @pl.loop(1, n + 1)
    def _(b):
        @pl.when(block_place(me, b) != me)
        def _():
            for h in range(PIECES):
                code_copy(b, h, partner).wait_send()

    for b, h in relayed:
        relay_in(b, h).wait_send()

    @pl.when(user_next(0) != me)
    def _():
        user_copy(0, partner).wait_send()

    @pl.when(odd_chip == 0)
    def _():
        bf_copy(0).wait_send()
        item_copy(0).wait_send()
        item_copy(strata - 1).wait_recv()

    last_item = pltpu.make_async_copy(items.at[strata], item_out, load_i)
    last_item.start()

    @pl.when(jnp.logical_or(core == 0, odd_chip == 1))
    def _():
        user_copy(strata - 1, partner).wait_recv()

    last_user = pltpu.make_async_copy(users.at[strata], user_out, load_u)
    last_user.start()

    @pl.when(user_next(strata - 1) != me)
    def _():
        user_copy(strata - 1, partner).wait_send()

    @pl.when(odd_chip == 0)
    def _():
        item_copy(strata - 1).wait_send()

    last_item.wait()
    last_user.wait()


def finish(user_in, item_in, user_out, item_out):
    user_out[...] = user_in[...]
    item_out[...] = item_in[...].T


def solution(mesh):
    n = mesh.shape["shard"]
    row_spec = P(("rep", "shard"), None)

    def local(ratings, observed, user_init, item_init):
        users_dev = ratings.shape[0]
        items_dev, rank = item_init.shape
        step_size = 0.5 / ((users_dev + items_dev + rank) / math.sqrt(rank))
        weight_decay = 0.03 * math.sqrt(users_dev * items_dev / rank)
        strata = EPOCHS * n
        relays = max(1, len(RELAY))
        vmem = pl.BlockSpec(memory_space=pltpu.VMEM)
        anywhere = pl.BlockSpec(memory_space=pl.ANY)
        dma = pltpu.SemaphoreType.DMA
        user_out, item_out = pl.pallas_call(
            functools.partial(kernel, n, step_size, weight_decay),
            out_shape=(
                jax.ShapeDtypeStruct((users_dev, rank), jnp.float32),
                jax.ShapeDtypeStruct((rank, items_dev), jnp.float32),
            ),
            in_specs=[anywhere] * 4,
            out_specs=(anywhere, anywhere),
            scratch_shapes=[
                pltpu.VMEM((n, users_dev, items_dev), jnp.float32),
                pltpu.VMEM((n, users_dev, items_dev), jnp.int32),
                pltpu.VMEM((n + 1, users_dev, items_dev), jnp.float32),
                pltpu.VMEM((n + 1, users_dev, items_dev), jnp.float32),
                pltpu.VMEM((relays, users_dev // PIECES, items_dev), jnp.float32),
                pltpu.VMEM((items_dev, rank), jnp.float32),
                pltpu.VMEM((strata + 1, rank, items_dev), jnp.float32),
                pltpu.VMEM((strata, rank, items_dev), jnp.bfloat16),
                pltpu.VMEM((strata + 1, users_dev, rank), jnp.float32),
                dma((n,)), dma((n,)), dma, dma, dma((n + 1, PIECES)), dma((n + 1, PIECES)), dma((relays,)), dma((relays,)),
                dma((strata,)), dma((strata,)), dma((strata,)), dma((strata,)), dma((strata,)), dma((strata,)),
            ],
            compiler_params=pltpu.CompilerParams(collective_id=0, has_side_effects=True),
        )(ratings, observed, user_init, item_init)
        return pl.pallas_call(
            finish,
            out_shape=(
                jax.ShapeDtypeStruct((users_dev, rank), jnp.float32),
                jax.ShapeDtypeStruct((items_dev, rank), jnp.float32),
            ),
            in_specs=[vmem, vmem],
            out_specs=(vmem, vmem),
        )(user_out, item_out)

    return jax.shard_map(local, mesh=mesh, in_specs=(row_spec,) * 4, out_specs=(row_spec, row_spec), check_vma=False)
```

```python
import functools
import math

import jax
import jax.numpy as jnp
from jax import lax
from jax.experimental import pallas as pl
from jax.experimental.pallas import tpu as pltpu
from jax.sharding import PartitionSpec as P

STRATUM_STEPS = 4
EPOCHS = 2
CORES = 2
PIECES = 1
SEND_AT = {(1, 0): 0, (2, 0): 1, (3, 0): 0, (4, 0): 2, (5, 0): 3, (6, 0): 5, (7, 0): 1, (8, 0): 3, (9, 0): 6, (10, 0): 0, (11, 0): 7, (12, 0): 7, (13, 0): 10, (14, 0): 12, (15, 0): 11, (16, 0): 12}
RELAY = {(7, 0): (4, 4), (8, 0): (4, 5)}
MESH = pl.DeviceIdType.MESH


def kernel(
    n, step_size, weight_decay, ratings, observed, user_in, item_in, user_out, item_out,
    rate_stage, seen_stage, code_send, code, relay, item_stage, items, items_bf, users,
    load_r, load_m, load_i, load_u, code_ss, code_rs, relay_ss, relay_rs, user_ss, user_rs,
    item_ss, item_rs, bf_ss, bf_rs,
):
    n_items = item_in.shape[0]
    rows = user_in.shape[0] // PIECES
    strata = EPOCHS * n
    chips = n // CORES
    me = lax.axis_index("shard")
    chip = me // CORES
    core = lax.rem(me, CORES)
    odd_chip = lax.rem(chip, 2)
    partner = me + 1 - 2 * core
    relayed = sorted(RELAY)

    def at(device):
        return {"shard": device}

    def shifted(offset):
        return at(lax.rem(me + n + offset, n))

    def block_place(owner, b):
        item = lax.rem(owner + b, n)
        return item - lax.rem(item, 2) + lax.rem(owner + item // 2, 2)

    def loads(b):
        col = pl.multiple_of(lax.rem(me + b, n) * n_items, n_items)
        slot = b % n
        return (
            pltpu.make_async_copy(ratings.at[:, pl.ds(col, n_items)], rate_stage.at[slot], load_r.at[slot]),
            pltpu.make_async_copy(observed.at[:, pl.ds(col, n_items)], seen_stage.at[slot], load_m.at[slot]),
        )

    def part(h):
        return pl.ds(h * rows, rows)

    def code_copy(b, h, device):
        return pltpu.make_async_remote_copy(
            src_ref=code_send.at[b, part(h)], dst_ref=code.at[b, part(h)], send_sem=code_ss.at[b, h],
            recv_sem=code_rs.at[b, h], device_id=at(device), device_id_type=MESH)

    def relay_in(b, h):
        r = relayed.index((b, h))
        return pltpu.make_async_remote_copy(
            src_ref=code_send.at[b, part(h)], dst_ref=relay.at[r], send_sem=relay_ss.at[r], recv_sem=relay_rs.at[r],
            device_id=shifted(-RELAY[b, h][0]), device_id_type=MESH)

    def relay_out(b, h):
        owner = lax.rem(me + RELAY[b, h][0], n)
        return pltpu.make_async_remote_copy(
            src_ref=relay.at[relayed.index((b, h))], dst_ref=code.at[b, part(h)], send_sem=code_ss.at[b, h],
            recv_sem=code_rs.at[b, h], device_id=at(block_place(owner, b)), device_id_type=MESH)

    def user_copy(t, device):
        return pltpu.make_async_remote_copy(
            src_ref=users.at[t], dst_ref=users.at[t + 1], send_sem=user_ss.at[t], recv_sem=user_rs.at[t],
            device_id=at(device), device_id_type=MESH)

    def bf_copy(t):
        return pltpu.make_async_remote_copy(
            src_ref=items_bf.at[t], dst_ref=items_bf.at[t + 1], send_sem=bf_ss.at[t], recv_sem=bf_rs.at[t],
            device_id=at(partner), device_id_type=MESH)

    def item_copy(t):
        return pltpu.make_async_remote_copy(
            src_ref=items.at[t], dst_ref=items.at[t + 1], send_sem=item_ss.at[t], recv_sem=item_rs.at[t],
            device_id=at(partner), device_id_type=MESH)

    def item_half(t):
        if isinstance(t, int) and t in (0, strata):
            return core
        return lax.rem(core + t + chip, 2)

    def user_next(t):
        half = item_half(t)
        up = lax.rem(chip + half, chips)
        if isinstance(t, int) and t + 1 == strata:
            return CORES * up + lax.rem(1 - half + t + 1, 2)
        return CORES * up + lax.rem(1 - half + t + 1 + up, 2)

    def owner_of(t):
        return lax.rem(CORES * chip + item_half(t) + strata - t, n)

    first_item = pltpu.make_async_copy(item_in, item_stage, load_i)
    first_user = pltpu.make_async_copy(user_in, users.at[0], load_u)

    def coded(b, h):
        return jnp.where(seen_stage[b % n, part(h)] != 0, rate_stage[b % n, part(h)], jnp.inf)

    def send_code(b, h):
        if b < n and all(SEND_AT[b, h] < SEND_AT[b, g] or (SEND_AT[b, h] == SEND_AT[b, g] and h <= g) for g in range(PIECES)):
            for load in loads(b):
                load.wait()
        if b in (1, n - 1, n):
            stays = block_place(me, b) == me

            @pl.when(stays)
            def _():
                code[b, part(h)] = coded(b, h)

            @pl.when(jnp.logical_not(stays))
            def _():
                code_send[b, part(h)] = coded(b, h)
                code_copy(b, h, block_place(me, b)).start()
        else:
            code_send[b, part(h)] = coded(b, h)
            if (b, h) in relayed:
                relay_in(b, h).start()
            else:
                code_copy(b, h, block_place(me, b)).start()

    def send_all(when):
        for b, h in sorted(SEND_AT):
            if SEND_AT[b, h] == when:
                send_code(b, h)

    def traffic(t):
        for when in sorted(set(SEND_AT.values()) - {0}):
            pl.when(t == when)(functools.partial(send_all, when))
        for b, h in relayed:
            @pl.when(t == RELAY[b, h][1])
            def _():
                relay_in(b, h).wait_recv()
                relay_out(b, h).start()

    barrier = pltpu.get_barrier_semaphore()
    for offset in range(1, n):
        pl.semaphore_signal(barrier, inc=1, device_id=shifted(offset), device_id_type=MESH)
    order = sorted(range(1, n), key=lambda b: min(SEND_AT[b, h] for h in range(PIECES)))
    early = [b for b in order if min(SEND_AT[b, h] for h in range(PIECES)) == 0]
    for b in early + [0]:
        for load in loads(b):
            load.start()
    first_item.start()
    first_user.start()
    for b in order[len(early):]:
        for load in loads(b):
            load.start()
    first_item.wait()
    first = item_stage[...].T
    items[0] = first
    items_bf[0] = first.astype(jnp.bfloat16)
    for load in loads(0):
        load.wait()
    for h in range(PIECES):
        code[0, part(h)] = coded(0, h)
    pl.semaphore_wait(barrier, n - 1)
    send_all(0)

    def stratum(t):
        fixed = isinstance(t, int)
        start, end = fixed and t == 0, fixed and t == strata - 1
        half = item_half(t)
        target = user_next(t)
        user_stays = target == me
        item_stays = odd_chip if start or end else 0
        user_from_far = half == 0
        if fixed and t == 1:
            user_from_far = jnp.logical_or(user_from_far, odd_chip == 1)
        item_swapped = odd_chip == 0 if fixed and t == 1 else None

        if not start and not (fixed and t > n):
            pl.when(t <= n)(functools.partial(traffic, t))

            @pl.when(jnp.logical_and(t <= n, owner_of(t) != me))
            def _():
                for h in range(PIECES):
                    code_copy(t, h, partner).wait_recv()

        if start:
            first_user.wait()
        else:
            @pl.when(user_from_far)
            def _():
                user_copy(t - 1, partner).wait_recv()

            if item_swapped is None:
                bf_copy(t - 1).wait_recv()
            else:
                @pl.when(item_swapped)
                def _():
                    bf_copy(t - 1).wait_recv()
                    item_copy(t - 1).wait_recv()

        slot = jnp.where(t > n, t - n, t)
        user = users[t]
        user_bf = user.astype(jnp.bfloat16)
        for step in range(STRATUM_STEPS):
            final = step == STRATUM_STEPS - 1
            pred = jnp.dot(user_bf, items_bf[t], preferred_element_type=jnp.float32)
            rate = code[slot]
            err = jnp.where(rate < jnp.inf, pred - rate, 0.0).astype(jnp.bfloat16)
            user = (1.0 - step_size * weight_decay) * user
            for h in range(2):
                cols = slice(h * n_items // 2, (h + 1) * n_items // 2)
                grad = lax.dot_general(
                    err[:, cols], items_bf[t, :, cols], (((1,), (1,)), ((), ())), preferred_element_type=jnp.float32)
                user = user - step_size * grad
            user_bf = user.astype(jnp.bfloat16)
            if final:
                users[t + user_stays.astype(jnp.int32)] = user

                @pl.when(jnp.logical_not(user_stays))
                def _():
                    user_copy(t, target).start()
            pred = jnp.dot(user_bf, items_bf[t], preferred_element_type=jnp.float32)
            rate = code[slot]
            err = jnp.where(rate < jnp.inf, pred - rate, 0.0).astype(jnp.bfloat16)
            grad = lax.dot_general(user_bf, err, (((0,), (0,)), ((), ())), preferred_element_type=jnp.float32)
            if step == 0 and not start and item_swapped is None:
                item_copy(t - 1).wait_recv()
            item = (1.0 - step_size * weight_decay) * items[t] - step_size * grad
            out = t + item_stays if final else t
            if not (final and end):
                items_bf[out] = item.astype(jnp.bfloat16)
            items[out] = item

        if start or end:
            @pl.when(item_stays == 0)
            def _():
                if start:
                    bf_copy(t).start()
                item_copy(t).start()
        else:
            bf_copy(t).start()
            item_copy(t).start()

    stratum(0)
    stratum(1)
    pl.loop(2, strata - 1)(stratum)
    stratum(strata - 1)

    def drain(t):
        @pl.when(user_next(t) != me)
        def _():
            user_copy(t, partner).wait_send()

        bf_copy(t).wait_send()
        item_copy(t).wait_send()

    pl.loop(1, strata - 1)(drain)

    @pl.loop(1, n + 1)
    def _(b):
        @pl.when(block_place(me, b) != me)
        def _():
            for h in range(PIECES):
                code_copy(b, h, partner).wait_send()

    for b, h in relayed:
        relay_in(b, h).wait_send()

    @pl.when(user_next(0) != me)
    def _():
        user_copy(0, partner).wait_send()

    @pl.when(odd_chip == 0)
    def _():
        bf_copy(0).wait_send()
        item_copy(0).wait_send()
        item_copy(strata - 1).wait_recv()

    last_item = pltpu.make_async_copy(items.at[strata], item_out, load_i)
    last_item.start()

    @pl.when(jnp.logical_or(core == 0, odd_chip == 1))
    def _():
        user_copy(strata - 1, partner).wait_recv()

    last_user = pltpu.make_async_copy(users.at[strata], user_out, load_u)
    last_user.start()

    @pl.when(user_next(strata - 1) != me)
    def _():
        user_copy(strata - 1, partner).wait_send()

    @pl.when(odd_chip == 0)
    def _():
        item_copy(strata - 1).wait_send()

    last_item.wait()
    last_user.wait()


def finish(user_in, item_in, user_out, item_out):
    user_out[...] = user_in[...]
    item_out[...] = item_in[...].T


def solution(mesh):
    n = mesh.shape["shard"]
    row_spec = P(("rep", "shard"), None)

    def local(ratings, observed, user_init, item_init):
        users_dev = ratings.shape[0]
        items_dev, rank = item_init.shape
        step_size = 0.5 / ((users_dev + items_dev + rank) / math.sqrt(rank))
        weight_decay = 0.03 * math.sqrt(users_dev * items_dev / rank)
        strata = EPOCHS * n
        relays = max(1, len(RELAY))
        vmem = pl.BlockSpec(memory_space=pltpu.VMEM)
        anywhere = pl.BlockSpec(memory_space=pl.ANY)
        dma = pltpu.SemaphoreType.DMA
        user_out, item_out = pl.pallas_call(
            functools.partial(kernel, n, step_size, weight_decay),
            out_shape=(
                jax.ShapeDtypeStruct((users_dev, rank), jnp.float32),
                jax.ShapeDtypeStruct((rank, items_dev), jnp.float32),
            ),
            in_specs=[anywhere] * 4,
            out_specs=(anywhere, anywhere),
            scratch_shapes=[
                pltpu.VMEM((n, users_dev, items_dev), jnp.float32),
                pltpu.VMEM((n, users_dev, items_dev), jnp.int32),
                pltpu.VMEM((n + 1, users_dev, items_dev), jnp.float32),
                pltpu.VMEM((n + 1, users_dev, items_dev), jnp.float32),
                pltpu.VMEM((relays, users_dev // PIECES, items_dev), jnp.float32),
                pltpu.VMEM((items_dev, rank), jnp.float32),
                pltpu.VMEM((strata + 1, rank, items_dev), jnp.float32),
                pltpu.VMEM((strata, rank, items_dev), jnp.bfloat16),
                pltpu.VMEM((strata + 1, users_dev, rank), jnp.float32),
                dma((n,)), dma((n,)), dma, dma, dma((n + 1, PIECES)), dma((n + 1, PIECES)), dma((relays,)), dma((relays,)),
                dma((strata,)), dma((strata,)), dma((strata,)), dma((strata,)), dma((strata,)), dma((strata,)),
            ],
            compiler_params=pltpu.CompilerParams(collective_id=0, has_side_effects=True),
        )(ratings, observed, user_init, item_init)
        return pl.pallas_call(
            finish,
            out_shape=(
                jax.ShapeDtypeStruct((users_dev, rank), jnp.float32),
                jax.ShapeDtypeStruct((items_dev, rank), jnp.float32),
            ),
            in_specs=[vmem, vmem],
            out_specs=(vmem, vmem),
        )(user_out, item_out)

    return jax.shard_map(local, mesh=mesh, in_specs=(row_spec,) * 4, out_specs=(row_spec, row_spec), check_vma=False)
```

```python
import functools
import math

import jax
import jax.numpy as jnp
from jax import lax
from jax.experimental import pallas as pl
from jax.experimental.pallas import tpu as pltpu
from jax.sharding import PartitionSpec as P

STRATUM_STEPS = 4
EPOCHS = 2
CORES = 2
TILES = 2
PIECES = 1
SEND_AT = {(1, 0): 0, (2, 0): 1, (3, 0): 0, (4, 0): 2, (5, 0): 3, (6, 0): 5, (7, 0): 1, (8, 0): 3, (9, 0): 6, (10, 0): 0, (11, 0): 7, (12, 0): 7, (13, 0): 10, (14, 0): 12, (15, 0): 11, (16, 0): 12}
RELAY = {(7, 0): (4, 4), (8, 0): (4, 5)}
MESH = pl.DeviceIdType.MESH


def kernel(
    n, step_size, weight_decay, ratings, observed, user_in, item_in, user_out, item_out,
    rate_stage, seen_stage, code_send, code, relay, item_stage, items, items_bf, users,
    load_r, load_m, load_i, load_u, code_ss, code_rs, relay_ss, relay_rs, user_ss, user_rs,
    item_ss, item_rs, bf_ss, bf_rs,
):
    n_items = item_in.shape[0]
    rows = user_in.shape[0] // PIECES
    strata = EPOCHS * n
    chips = n // CORES
    me = lax.axis_index("shard")
    chip = me // CORES
    core = lax.rem(me, CORES)
    odd_chip = lax.rem(chip, 2)
    partner = me + 1 - 2 * core
    relayed = sorted(RELAY)

    def at(device):
        return {"shard": device}

    def shifted(offset):
        return at(lax.rem(me + n + offset, n))

    def block_place(owner, b):
        item = lax.rem(owner + b, n)
        return item - lax.rem(item, 2) + lax.rem(owner + item // 2, 2)

    def loads(b):
        col = pl.multiple_of(lax.rem(me + b, n) * n_items, n_items)
        slot = b % n
        return (
            pltpu.make_async_copy(ratings.at[:, pl.ds(col, n_items)], rate_stage.at[slot], load_r.at[slot]),
            pltpu.make_async_copy(observed.at[:, pl.ds(col, n_items)], seen_stage.at[slot], load_m.at[slot]),
        )

    def part(h):
        return pl.ds(h * rows, rows)

    def code_copy(b, h, device):
        return pltpu.make_async_remote_copy(
            src_ref=code_send.at[b, part(h)], dst_ref=code.at[b, part(h)], send_sem=code_ss.at[b, h],
            recv_sem=code_rs.at[b, h], device_id=at(device), device_id_type=MESH)

    def relay_in(b, h):
        r = relayed.index((b, h))
        return pltpu.make_async_remote_copy(
            src_ref=code_send.at[b, part(h)], dst_ref=relay.at[r], send_sem=relay_ss.at[r], recv_sem=relay_rs.at[r],
            device_id=shifted(-RELAY[b, h][0]), device_id_type=MESH)

    def relay_out(b, h):
        owner = lax.rem(me + RELAY[b, h][0], n)
        return pltpu.make_async_remote_copy(
            src_ref=relay.at[relayed.index((b, h))], dst_ref=code.at[b, part(h)], send_sem=code_ss.at[b, h],
            recv_sem=code_rs.at[b, h], device_id=at(block_place(owner, b)), device_id_type=MESH)

    def user_copy(t, device):
        return pltpu.make_async_remote_copy(
            src_ref=users.at[t], dst_ref=users.at[t + 1], send_sem=user_ss.at[t], recv_sem=user_rs.at[t],
            device_id=at(device), device_id_type=MESH)

    def bf_copy(t):
        return pltpu.make_async_remote_copy(
            src_ref=items_bf.at[t], dst_ref=items_bf.at[t + 1], send_sem=bf_ss.at[t], recv_sem=bf_rs.at[t],
            device_id=at(partner), device_id_type=MESH)

    def item_copy(t):
        return pltpu.make_async_remote_copy(
            src_ref=items.at[t], dst_ref=items.at[t + 1], send_sem=item_ss.at[t], recv_sem=item_rs.at[t],
            device_id=at(partner), device_id_type=MESH)

    def item_half(t):
        if isinstance(t, int) and t in (0, strata):
            return core
        return lax.rem(core + t + chip, 2)

    def user_next(t):
        half = item_half(t)
        up = lax.rem(chip + half, chips)
        if isinstance(t, int) and t + 1 == strata:
            return CORES * up + lax.rem(1 - half + t + 1, 2)
        return CORES * up + lax.rem(1 - half + t + 1 + up, 2)

    def owner_of(t):
        return lax.rem(CORES * chip + item_half(t) + strata - t, n)

    first_item = pltpu.make_async_copy(item_in, item_stage, load_i)
    first_user = pltpu.make_async_copy(user_in, users.at[0], load_u)

    def coded(b, h):
        return jnp.where(seen_stage[b % n, part(h)] != 0, rate_stage[b % n, part(h)], jnp.inf)

    def send_code(b, h):
        if b < n and all(SEND_AT[b, h] < SEND_AT[b, g] or (SEND_AT[b, h] == SEND_AT[b, g] and h <= g) for g in range(PIECES)):
            for load in loads(b):
                load.wait()
        if b in (1, n - 1, n):
            stays = block_place(me, b) == me

            @pl.when(stays)
            def _():
                code[b, part(h)] = coded(b, h)

            @pl.when(jnp.logical_not(stays))
            def _():
                code_send[b, part(h)] = coded(b, h)
                code_copy(b, h, block_place(me, b)).start()
        else:
            code_send[b, part(h)] = coded(b, h)
            if (b, h) in relayed:
                relay_in(b, h).start()
            else:
                code_copy(b, h, block_place(me, b)).start()

    def send_all(when):
        for b, h in sorted(SEND_AT):
            if SEND_AT[b, h] == when:
                send_code(b, h)

    def traffic(t):
        for when in sorted(set(SEND_AT.values()) - {0}):
            pl.when(t == when)(functools.partial(send_all, when))
        for b, h in relayed:
            @pl.when(t == RELAY[b, h][1])
            def _():
                relay_in(b, h).wait_recv()
                relay_out(b, h).start()

    barrier = pltpu.get_barrier_semaphore()
    for offset in range(1, n):
        pl.semaphore_signal(barrier, inc=1, device_id=shifted(offset), device_id_type=MESH)
    order = sorted(range(1, n), key=lambda b: min(SEND_AT[b, h] for h in range(PIECES)))
    early = [b for b in order if min(SEND_AT[b, h] for h in range(PIECES)) == 0]
    for b in early + [0]:
        for load in loads(b):
            load.start()
    first_item.start()
    first_user.start()
    for b in order[len(early):]:
        for load in loads(b):
            load.start()
    first_item.wait()
    first = item_stage[...].T
    items[0] = first
    items_bf[0] = first.astype(jnp.bfloat16)
    for load in loads(0):
        load.wait()
    for h in range(PIECES):
        code[0, part(h)] = coded(0, h)
    pl.semaphore_wait(barrier, n - 1)
    send_all(0)

    def stratum(t):
        fixed = isinstance(t, int)
        start, end = fixed and t == 0, fixed and t == strata - 1
        half = item_half(t)
        target = user_next(t)
        user_stays = target == me
        item_stays = odd_chip if start or end else 0
        user_from_far = half == 0
        if fixed and t == 1:
            user_from_far = jnp.logical_or(user_from_far, odd_chip == 1)
        item_swapped = odd_chip == 0 if fixed and t == 1 else None

        if not start and not (fixed and t > n):
            pl.when(t <= n)(functools.partial(traffic, t))

            @pl.when(jnp.logical_and(t <= n, owner_of(t) != me))
            def _():
                for h in range(PIECES):
                    code_copy(t, h, partner).wait_recv()

        if start:
            first_user.wait()
        else:
            @pl.when(user_from_far)
            def _():
                user_copy(t - 1, partner).wait_recv()

            if item_swapped is None:
                bf_copy(t - 1).wait_recv()
            else:
                @pl.when(item_swapped)
                def _():
                    bf_copy(t - 1).wait_recv()
                    item_copy(t - 1).wait_recv()

        slot = jnp.where(t > n, t - n, t)
        user = users[t]
        user_bf = user.astype(jnp.bfloat16)
        for step in range(STRATUM_STEPS):
            final = step == STRATUM_STEPS - 1
            pred = jnp.dot(user_bf, items_bf[t], preferred_element_type=jnp.float32)
            rate = code[slot]
            err = jnp.where(rate < jnp.inf, pred - rate, 0.0).astype(jnp.bfloat16)
            user = (1.0 - step_size * weight_decay) * user
            for h in range(2):
                cols = slice(h * n_items // 2, (h + 1) * n_items // 2)
                grad = lax.dot_general(
                    err[:, cols], items_bf[t, :, cols], (((1,), (1,)), ((), ())), preferred_element_type=jnp.float32)
                user = user - step_size * grad
            user_bf = user.astype(jnp.bfloat16)
            if final:
                users[t + user_stays.astype(jnp.int32)] = user

                @pl.when(jnp.logical_not(user_stays))
                def _():
                    user_copy(t, target).start()
            pred = jnp.dot(user_bf, items_bf[t], preferred_element_type=jnp.float32)
            rate = code[slot]
            err = jnp.where(rate < jnp.inf, pred - rate, 0.0).astype(jnp.bfloat16)
            grad = lax.dot_general(user_bf, err, (((0,), (0,)), ((), ())), preferred_element_type=jnp.float32)
            if step == 0 and not start and item_swapped is None:
                item_copy(t - 1).wait_recv()
            item = (1.0 - step_size * weight_decay) * items[t] - step_size * grad
            out = t + item_stays if final else t
            if not (final and end):
                items_bf[out] = item.astype(jnp.bfloat16)
            items[out] = item

        if start or end:
            @pl.when(item_stays == 0)
            def _():
                if start:
                    bf_copy(t).start()
                item_copy(t).start()
        else:
            bf_copy(t).start()
            item_copy(t).start()

    stratum(0)
    stratum(1)
    pl.loop(2, strata - 1)(stratum)
    stratum(strata - 1)

    def drain(t):
        @pl.when(user_next(t) != me)
        def _():
            user_copy(t, partner).wait_send()

        bf_copy(t).wait_send()
        item_copy(t).wait_send()

    pl.loop(1, strata - 1)(drain)

    @pl.loop(1, n + 1)
    def _(b):
        @pl.when(block_place(me, b) != me)
        def _():
            for h in range(PIECES):
                code_copy(b, h, partner).wait_send()

    for b, h in relayed:
        relay_in(b, h).wait_send()

    @pl.when(user_next(0) != me)
    def _():
        user_copy(0, partner).wait_send()

    @pl.when(odd_chip == 0)
    def _():
        bf_copy(0).wait_send()
        item_copy(0).wait_send()
        item_copy(strata - 1).wait_recv()

    last_item = pltpu.make_async_copy(items.at[strata], item_out, load_i)
    last_item.start()

    @pl.when(jnp.logical_or(core == 0, odd_chip == 1))
    def _():
        user_copy(strata - 1, partner).wait_recv()

    last_user = pltpu.make_async_copy(users.at[strata], user_out, load_u)
    last_user.start()

    @pl.when(user_next(strata - 1) != me)
    def _():
        user_copy(strata - 1, partner).wait_send()

    @pl.when(odd_chip == 0)
    def _():
        item_copy(strata - 1).wait_send()

    last_item.wait()
    last_user.wait()


def finish(user_in, item_in, user_out, item_out):
    user_out[...] = user_in[...]
    item_out[...] = item_in[...].T


def solution(mesh):
    n = mesh.shape["shard"]
    row_spec = P(("rep", "shard"), None)

    def local(ratings, observed, user_init, item_init):
        users_dev = ratings.shape[0]
        items_dev, rank = item_init.shape
        step_size = 0.5 / ((users_dev + items_dev + rank) / math.sqrt(rank))
        weight_decay = 0.03 * math.sqrt(users_dev * items_dev / rank)
        strata = EPOCHS * n
        relays = max(1, len(RELAY))
        vmem = pl.BlockSpec(memory_space=pltpu.VMEM)
        anywhere = pl.BlockSpec(memory_space=pl.ANY)
        dma = pltpu.SemaphoreType.DMA
        user_out, item_out = pl.pallas_call(
            functools.partial(kernel, n, step_size, weight_decay),
            out_shape=(
                jax.ShapeDtypeStruct((users_dev, rank), jnp.float32),
                jax.ShapeDtypeStruct((rank, items_dev), jnp.float32),
            ),
            in_specs=[anywhere] * 4,
            out_specs=(anywhere, anywhere),
            scratch_shapes=[
                pltpu.VMEM((n, users_dev, items_dev), jnp.float32),
                pltpu.VMEM((n, users_dev, items_dev), jnp.int32),
                pltpu.VMEM((n + 1, users_dev, items_dev), jnp.float32),
                pltpu.VMEM((n + 1, users_dev, items_dev), jnp.float32),
                pltpu.VMEM((relays, users_dev // PIECES, items_dev), jnp.float32),
                pltpu.VMEM((items_dev, rank), jnp.float32),
                pltpu.VMEM((strata + 1, rank, items_dev), jnp.float32),
                pltpu.VMEM((strata, rank, items_dev), jnp.bfloat16),
                pltpu.VMEM((strata + 1, users_dev, rank), jnp.float32),
                dma((n,)), dma((n,)), dma, dma, dma((n + 1, PIECES)), dma((n + 1, PIECES)), dma((relays,)), dma((relays,)),
                dma((strata,)), dma((strata,)), dma((strata,)), dma((strata,)), dma((strata,)), dma((strata,)),
            ],
            compiler_params=pltpu.CompilerParams(collective_id=0, has_side_effects=True),
        )(ratings, observed, user_init, item_init)
        return pl.pallas_call(
            finish,
            out_shape=(
                jax.ShapeDtypeStruct((users_dev, rank), jnp.float32),
                jax.ShapeDtypeStruct((items_dev, rank), jnp.float32),
            ),
            grid=(TILES,),
            in_specs=[
                pl.BlockSpec((users_dev // TILES, rank), lambda i: (i, 0)),
                pl.BlockSpec((rank, items_dev // TILES), lambda i: (0, i)),
            ],
            out_specs=(
                pl.BlockSpec((users_dev // TILES, rank), lambda i: (i, 0)),
                pl.BlockSpec((items_dev // TILES, rank), lambda i: (i, 0)),
            ),
        )(user_out, item_out)

    return jax.shard_map(local, mesh=mesh, in_specs=(row_spec,) * 4, out_specs=(row_spec, row_spec), check_vma=False)
```
